32 devices in a mesh: tok: 16 (over z, y, x), col: 2 (over core).
Axes of the slice: x: 2, y: 2, z: 4, core: 2. Of those that a mesh axis runs over, the one named last changes fastest.
Arguments:
- first_acts: bfloat16 [24576, 4096], P('tok', 'col'), as said below
- second_acts: bfloat16 [24576, 4096], P('tok', 'col'), as said below
- window_counts: int32 [64], P('tok'), may hold values from 96 to 384, as said below
Outputs:
- whitened: float32 [4096, 4096], P('tok', 'col')
- means: float32 [2, 4096], P(None, 'col')
The draws below stay inside these ranges and needn't reach their ends.
Inputs may be any that keep to these rules, and one draw needn't show every extreme that they name: `window_counts`: the live tokens of a window are its first ones; on every index of tok one of its 4 windows is full with 384 live tokens. `first_acts`: real values of order one to some tens; slots that are not live hold values too. `second_acts`: real values of order one to some tens; slots that are not live hold values too.
All inputs are finite; a program needn't handle non-finite values.
Results may differ from the reference program's by a relative error of at most 0.0003.
Values may be sent and summed in bfloat16 or wider, within the bound.
No kernel may reach another device: no remote copies, remote signals or barrier semaphores. Data moves between devices by JAX's collectives and lax.ppermute only.
A program may use at most 192 MiB of HBM per device.

```python
import math
import jax
import jax.numpy as jnp
from jax import lax

D = 4096
WINDOWS = 4
SLOTS = 384
TOK_DEV = 1536
TOKENS = 24576
BLOCKS = 64
N_TOK = 16


def paired_draw(key):
    key = jax.random.fold_in(key, 11)
    streams = jax.random.split(key, 8)
    feature_block = D // N_TOK
    base_field = jax.random.normal(streams[0], (TOKENS, D), jnp.float32)
    noise_field = jax.random.normal(streams[1], (TOKENS, D), jnp.float32)
    offset_scale = 1.0
    common_shift = 0.0
    row_scale = jnp.ones((TOKENS,), jnp.float32)
    channel_scale = jnp.exp(jax.random.uniform(streams[2], (D,), jnp.float32, math.log(0.5), math.log(2.0)))
    block_shift = offset_scale * jax.random.normal(streams[3], (BLOCKS, D), jnp.float32) + common_shift
    second_shift = offset_scale * jax.random.normal(streams[6], (BLOCKS, D), jnp.float32)
    pairing = jax.random.permutation(streams[4], N_TOK)
    row_device = jnp.arange(TOKENS, dtype=jnp.int32) // TOK_DEV
    feature_owner = jnp.arange(D, dtype=jnp.int32) // feature_block
    spike_scale = jnp.where(pairing[row_device][:, None] == feature_owner[None, :], 5.0, 1.0)
    first_field = (base_field * channel_scale[None, :] * row_scale[:, None] + jnp.repeat(block_shift, SLOTS, axis=0)) * spike_scale
    second_field = 0.5 * first_field + 0.4 * jnp.roll(first_field, 1, axis=1) + 0.6 * noise_field * channel_scale[None, :] + jnp.repeat(second_shift, SLOTS, axis=0)
    return (first_field, second_field)


def draw_first_acts(key, part):
    return paired_draw(key)[0].astype(jnp.bfloat16)


def draw_second_acts(key, part):
    return paired_draw(key)[1].astype(jnp.bfloat16)


def draw_window_counts(key, part):
    key_counts, key_full = jax.random.split(jax.random.fold_in(key, 29))
    drawn = jax.random.randint(key_counts, (BLOCKS,), SLOTS // 4, SLOTS + 1, jnp.int32)
    chosen = jax.random.randint(key_full, (N_TOK,), 0, WINDOWS, jnp.int32)
    filled = (lax_iota_windows()[None, :] == chosen[:, None]).reshape(BLOCKS)
    return jnp.where(filled, SLOTS, drawn).astype(jnp.int32)


def lax_iota_windows():
    return jnp.arange(WINDOWS, dtype=jnp.int32)


def setup_inputs(seed: int = 0) -> dict:
    key_of = jax.random.split(jax.random.key(seed), 4)
    first_acts = draw_first_acts(jax.random.fold_in(key_of[3], 71), 0)
    second_acts = draw_second_acts(jax.random.fold_in(key_of[3], 71), 0)
    window_counts = draw_window_counts(jax.random.fold_in(key_of[3], 71), 0)
    return {"first_acts": first_acts, "second_acts": second_acts, "window_counts": window_counts}


def reference(first_acts, second_acts, window_counts):
    blocks = window_counts.shape[0]
    first_win = first_acts.reshape(blocks, SLOTS, D)
    second_win = second_acts.reshape(blocks, SLOTS, D)
    live_mask = lax.broadcasted_iota(jnp.int32, (blocks, SLOTS), 1) < window_counts[:, None]
    count_float = window_counts.astype(jnp.float32)
    mean_first = lax.optimization_barrier(jnp.sum(jnp.where(live_mask[:, :, None], first_win.astype(jnp.float32), 0.0), axis=1)) / count_float[:, None]
    mean_second = lax.optimization_barrier(jnp.sum(jnp.where(live_mask[:, :, None], second_win.astype(jnp.float32), 0.0), axis=1)) / count_float[:, None]
    grand_count = jnp.sum(count_float)
    grand_first = lax.optimization_barrier(jnp.sum(count_float[:, None] * mean_first, axis=0)) / grand_count
    grand_second = lax.optimization_barrier(jnp.sum(count_float[:, None] * mean_second, axis=0)) / grand_count

    def accumulate(carry, inputs):
        cross, square_first, square_second = carry
        rows_first, rows_second, live_rows, win_first, win_second = inputs
        centered_first = jnp.where(live_rows[:, None], rows_first - win_first[None, :], 0.0).astype(jnp.bfloat16)
        centered_second = jnp.where(live_rows[:, None], rows_second - win_second[None, :], 0.0).astype(jnp.bfloat16)
        cross = cross + jnp.dot(centered_first.T, centered_second, preferred_element_type=jnp.float32)
        square_first = square_first + lax.optimization_barrier(jnp.sum(jnp.square(centered_first.astype(jnp.float32)), axis=0))
        square_second = square_second + lax.optimization_barrier(jnp.sum(jnp.square(centered_second.astype(jnp.float32)), axis=0))
        return ((cross, square_first, square_second), None)
    start_state = (jnp.zeros((D, D), jnp.float32), jnp.zeros((D,), jnp.float32), jnp.zeros((D,), jnp.float32))
    (cross, square_first, square_second), _ = lax.scan(accumulate, start_state, (first_win, second_win, live_mask, mean_first, mean_second))
    shift_first = mean_first - grand_first[None, :]
    shift_second = mean_second - grand_second[None, :]
    cross = cross + jnp.dot((count_float[:, None] * shift_first).T, shift_second, preferred_element_type=jnp.float32, precision=lax.Precision.HIGHEST)
    var_first = (square_first + lax.optimization_barrier(jnp.sum(count_float[:, None] * jnp.square(shift_first), axis=0))) / grand_count
    var_second = (square_second + lax.optimization_barrier(jnp.sum(count_float[:, None] * jnp.square(shift_second), axis=0))) / grand_count
    whitened = cross / grand_count / jnp.sqrt((var_first[:, None] + 0.1) * (var_second[None, :] + 0.1))
    means = jnp.stack([grand_first, grand_second])
    return (whitened, means)
```

```python
import functools
import math

import jax
import jax.numpy as jnp
from jax import lax
from jax.experimental import pallas as pl
from jax.experimental.pallas import tpu as pltpu
from jax.sharding import PartitionSpec as P


SEND = jnp.float16


def ring_label(index, ring_mask):
    return index ^ ((index >> 1) & ring_mask)


def split_columns(width, parts):
    units = width // 128
    edges = [(units * p // parts) * 128 for p in range(parts + 1)]
    return list(zip(edges[:-1], edges[1:]))


def product_body(order_ref, left_ref, right_ref, out_ref, *, scale):
    product = lax.dot_general(
        left_ref[...], right_ref[...], (((1,), (0,)), ((), ())), preferred_element_type=jnp.float32
    )
    out_ref[...] = (product * scale).astype(out_ref.dtype)


def block_product(order, left, right, block, scale, dtype):
    rows = order.shape[0]
    tokens, width = right.shape
    return pl.pallas_call(
        functools.partial(product_body, scale=scale),
        out_shape=jax.ShapeDtypeStruct((rows * block, width), dtype),
        grid_spec=pltpu.PrefetchScalarGridSpec(
            num_scalar_prefetch=1,
            grid=(rows,),
            in_specs=[
                pl.BlockSpec((block, tokens), lambda i, order_ref: (order_ref[i], 0)),
                pl.BlockSpec((tokens, width), lambda i, order_ref: (0, 0)),
            ],
            out_specs=pl.BlockSpec((block, width), lambda i, order_ref: (i, 0)),
        ),
        compiler_params=pltpu.CompilerParams(dimension_semantics=("arbitrary",)),
    )(order, left, right)


def local(first_acts, second_acts, window_counts):
    windows = window_counts.shape[0]
    tokens, half_width = first_acts.shape
    slot_count = tokens // windows
    col_index = lax.axis_index("col")
    tok_index = lax.axis_index("tok")
    n_tok = lax.axis_size("tok")
    full_width = half_width * lax.axis_size("col")
    row_width = full_width // n_tok
    bits = n_tok.bit_length() - 1
    ring_mask = sum(1 << b for b in range(0, bits, 2)) if bits % 3 == 0 else 1 << (bits - 2)
    scale = 2.0 ** -math.ceil(math.log2(tokens * n_tok))

    count_float = window_counts.astype(jnp.float32)
    live_mask = lax.broadcasted_iota(jnp.int32, (windows, slot_count), 1) < window_counts[:, None]
    mask_half = live_mask.astype(jnp.bfloat16)
    first_win = first_acts.reshape(windows, slot_count, half_width)
    second_win = second_acts.reshape(windows, slot_count, half_width)

    def window_mean(win):
        total = jnp.einsum("ws,wsd->wd", mask_half, win, preferred_element_type=jnp.float32)
        return total / count_float[:, None]

    def center(win, mean):
        centered = jnp.where(live_mask[:, :, None], win - mean[:, None, :], 0.0)
        return centered.astype(jnp.bfloat16).reshape(tokens, half_width)

    mean_first = window_mean(first_win)
    centered_first = center(first_win, mean_first)
    left = lax.all_gather(centered_first.T, "col", axis=0, tiled=True)
    mean_second = window_mean(second_win)
    centered_second = center(second_win, mean_second)

    columns = split_columns(half_width, bits)
    rights = [centered_second[:, a:b] for a, b in columns]
    half = n_tok // 2
    orders = []
    dims = []
    for p in range(bits):
        order = [(p + j) % bits for j in range(bits)]
        labels = []
        for q in range(n_tok):
            s = sum(1 << order[j] for j in range(bits) if (q >> (bits - 1 - j)) & 1)
            labels.append(ring_label(s, ring_mask))
        orders.append(tok_index ^ jnp.array(labels, jnp.int32))
        dims.append([ring_label(1 << d, ring_mask) for d in order])

    def exchange(x, flip):
        return lax.ppermute(x, "tok", [(t, t ^ flip) for t in range(n_tok)])

    received = []
    for p in range(bits):
        sent = block_product(orders[p][half:], left, rights[p], row_width, scale, jnp.float32).astype(SEND)
        received.append(exchange(sent, dims[p][0]))
    kept = [
        block_product(orders[p][:half], left, rights[p], row_width, scale, jnp.float32)
        for p in range(bits)
    ]

    square_first = jnp.sum(jnp.square(centered_first.astype(jnp.float32)), axis=0)
    square_second = jnp.sum(jnp.square(centered_second.astype(jnp.float32)), axis=0)
    count_row = jnp.zeros((1, half_width), jnp.float32).at[0, :windows].set(count_float)
    stats = jnp.concatenate(
        [mean_first, mean_second, square_first[None], square_second[None], count_row], axis=0
    )
    peers = lax.all_gather(stats, "tok", axis=0)
    all_first = peers[:, :windows].reshape(n_tok * windows, half_width)
    all_second = peers[:, windows : 2 * windows].reshape(n_tok * windows, half_width)
    all_count = peers[:, 2 * windows + 2, :windows].reshape(n_tok * windows)
    grand_count = jnp.sum(all_count)
    grand_first = jnp.sum(all_count[:, None] * all_first, axis=0) / grand_count
    grand_second = jnp.sum(all_count[:, None] * all_second, axis=0) / grand_count
    shift_first = all_first - grand_first[None, :]
    shift_second = all_second - grand_second[None, :]
    var_first = (
        jnp.sum(peers[:, 2 * windows], axis=0)
        + jnp.sum(all_count[:, None] * jnp.square(shift_first), axis=0)
    ) / grand_count
    var_second = (
        jnp.sum(peers[:, 2 * windows + 1], axis=0)
        + jnp.sum(all_count[:, None] * jnp.square(shift_second), axis=0)
    ) / grand_count
    row_start = tok_index * row_width
    owner = row_start // half_width
    row_side = lax.dynamic_slice_in_dim(
        jnp.concatenate([all_count[:, None] * shift_first, var_first[None]], axis=0),
        row_start - owner * half_width,
        row_width,
        1,
    )
    row_side = lax.psum(jnp.where(owner == col_index, row_side, 0.0), "col")
    between = lax.dot_general(
        row_side[:-1],
        shift_second,
        (((0,), (0,)), ((), ())),
        precision=lax.Precision.HIGHEST,
        preferred_element_type=jnp.float32,
    )
    denominator = jnp.sqrt((row_side[-1][:, None] + 0.1) * (var_second[None, :] + 0.1))

    current = list(kept)
    for j in range(1, bits):
        rows = current[0].shape[0] // 2
        arriving = []
        for p in range(bits):
            total = current[p][rows:] + received[p][rows:].astype(jnp.float32)
            arriving.append(exchange(total.astype(SEND), dims[p][j]))
        current = [
            current[p][:rows] + received[p][:rows].astype(jnp.float32) for p in range(bits)
        ]
        received = arriving
    within = jnp.concatenate(
        [current[p] + received[p].astype(jnp.float32) for p in range(bits)], axis=1
    )
    cross = within * (1.0 / scale) + between
    whitened = cross / grand_count / denominator
    means = jnp.stack([grand_first, grand_second])
    return (whitened, means)


def solution(mesh):
    placed = (P("tok", "col"), P("tok", "col"), P("tok"))
    return jax.shard_map(
        local,
        mesh=mesh,
        in_specs=placed,
        out_specs=(P("tok", "col"), P(None, "col")),
        check_vma=False,
    )
```
